32 devices in a mesh: band: 8 (over z, core), grid: 4 (over y, x).
Axes of the slice: x: 2, y: 2, z: 4, core: 2. Of those that a mesh axis runs over, the one named last changes fastest.
Arguments:
- orbitals: bfloat16 [16, 192, 192, 192], P('band', 'grid'), may hold values from -6 to 6
- plan: int32 [2, 16], P(None, 'band'), may hold values from 0 to 1
Outputs:
- exchange_image: bfloat16 [16, 192, 192, 192], P('band', 'grid')
The draws below stay inside these ranges and needn't reach their ends.
Inputs may be any that keep to these rules, and one draw needn't show every extreme that they name: plan[s, i] is the position, within the partner group of band i at shift s + 1, of the band that band i pairs with.
All inputs are finite; a program needn't handle non-finite values.
Results may differ from the reference program's by a relative error of at most 0.0095.
Values may be sent and summed in bfloat16 or wider, within the bound.
A program may use at most 192 MiB of HBM per device.

```python
import jax
import jax.numpy as jnp
from jax import lax

NG = 192
B_DEV = 2
SHIFTS = 2
BANDS = 16
N_BAND = 8


def with_ends(entries, key, smallest, high):
    shape = entries.shape
    spot = [jax.random.randint(jax.random.fold_in(key, axis), (), 0, shape[axis]) for axis in range(len(shape))]
    entries = entries.at[tuple(spot)].set(smallest)
    longest = shape.index(max(shape))
    spot[longest] = (spot[longest] + 1) % shape[longest]
    return entries.at[tuple(spot)].set(high)


def level_of(key, dims, split, least, top_value):
    loudness = 1.0
    for dim, shards_of in split:
        draws = jax.random.uniform(jax.random.fold_in(jax.random.fold_in(key, 6), dim), (shards_of,), jnp.float32, least / len(split), top_value / len(split))
        loudness = loudness * jnp.repeat(jnp.exp(draws), dims[dim] // shards_of).reshape((-1,) + (1,) * (len(dims) - 1 - dim))
    return loudness


def noise(rng, dims, deviation, reach, shards=(), held_as=jnp.bfloat16):
    values = jax.random.normal(rng, dims, jnp.float32) * deviation
    if len(shards) > 0:
        values = level_of(rng, dims, shards, -0.22, 0.18) * values
    return jnp.clip(values, min=-reach, max=reach).astype(held_as)


def setup_inputs(seed: int = 0) -> dict:
    key_list = jax.random.split(jax.random.key(seed), 3)
    return {
        "orbitals": noise(key_list[0], (BANDS, NG, NG, NG), 1.0, 6.0, ((0, 8), (1, 4))),
        "plan": with_ends(jax.random.randint(key_list[1], (SHIFTS, BANDS), 0, B_DEV), jax.random.fold_in(key_list[1], 1), 0, B_DEV - 1).astype(jnp.int32),
    }


screening = 0.0005


def sine_table(length):
    counts = jnp.arange(1, length + 1, dtype=jnp.float32)
    return jnp.sin(jnp.pi * counts[:, None] * counts[None, :] / (length + 1)).astype(jnp.bfloat16)


def eigen_line(modes, length):
    return 2.0 - 2.0 * jnp.cos(jnp.pi * modes / (length + 1))


def rounded(values):
    return lax.optimization_barrier(values.astype(jnp.bfloat16)).astype(jnp.float32)


def solve(density, table, kernel):
    high = lax.Precision.HIGHEST
    field = density.astype(jnp.float32)
    section = rounded(jnp.einsum("xyz,kz->xyk", field, table, precision=high))
    section = rounded(jnp.einsum("xyz,ky->xkz", section, table, precision=high))
    spectrum = jnp.einsum("xyz,kx->kyz", section, table, precision=high)
    section = rounded(spectrum * kernel)
    section = rounded(jnp.einsum("xyz,kx->kyz", section, table, precision=high))
    section = rounded(jnp.einsum("xyz,ky->xkz", section, table, precision=high))
    return jnp.einsum("xyz,kz->xyk", section, table, precision=high)


def reference(orbitals, plan):
    band_count = orbitals.shape[0]
    length = orbitals.shape[1]
    per_group = band_count // N_BAND
    table = sine_table(length).astype(jnp.float32)
    modes = jnp.arange(1, length + 1, dtype=jnp.float32)
    line = eigen_line(modes, length)
    kernel = (2.0 / (length + 1)) ** 3 / (line[:, None, None] + line[None, :, None] + line[None, None, :] + screening)
    own_sums = jnp.zeros(orbitals.shape, jnp.float32)
    for offset in range(1, SHIFTS + 1):
        def step(carry, index):
            own_acc, partner_acc = carry
            group = index // per_group
            partner = (((group + offset) % N_BAND) * per_group + plan[offset - 1, index]).astype(jnp.int32)
            first_band = orbitals[index].astype(jnp.float32)
            second_band = orbitals[partner].astype(jnp.float32)
            density = (first_band * second_band).astype(jnp.bfloat16)
            potential = solve(density, table, kernel)
            own_acc = own_acc.at[index].add(potential * second_band)
            partner_acc = partner_acc.at[partner].add(potential * first_band)
            return (own_acc, partner_acc), None

        partner_zero = jnp.zeros(orbitals.shape, jnp.float32)
        (own_sums, partner_sums), _ = lax.scan(step, (own_sums, partner_zero), jnp.arange(band_count, dtype=jnp.int32))
        own_sums = own_sums + rounded(partner_sums)
    return (-own_sums).astype(jnp.bfloat16)
```

```python
import functools

import jax
import jax.numpy as jnp
from jax import lax
from jax.experimental import pallas as pl
from jax.experimental.pallas import tpu as pltpu
from jax.sharding import PartitionSpec as P


CHUNKS = 4
PACK = True

screening = 0.0005
TILE = 16


def routed(block, axis, target):
    return lax.ppermute(block, axis, [(i, target(i)) for i in range(lax.axis_size(axis))])


def packed_send(block, axis, target):
    parts = block.shape[0]
    length = block.shape[-1]
    if not PACK or length % 128 == 0 or (2 * length) % 128 or parts % 2:
        return routed(block, axis, target)
    half = parts // 2
    wide = jnp.concatenate([block[:half], block[half:]], axis=-1)
    got = routed(wide, axis, target)
    return jnp.concatenate([got[..., :length], got[..., length:]], axis=0)


def sine_table(length):
    counts = jnp.arange(1, length + 1, dtype=jnp.float32)
    return jnp.sin(jnp.pi * counts[:, None] * counts[None, :] / (length + 1)).astype(jnp.bfloat16)


def eigen_line(modes, length):
    return 2.0 - 2.0 * jnp.cos(jnp.pi * modes / (length + 1))


def plain_shards(orbitals, plan):
    per_group, planes, _, length = orbitals.shape
    grid = lax.axis_size("grid")
    bands = lax.axis_size("band")
    me = lax.axis_index("grid")
    even = lax.axis_index("band") % 2 == 0
    columns = length // grid
    chunks = CHUNKS if planes % CHUNKS == 0 else 1
    width = planes // chunks

    def peer(i, r):
        return i ^ r if grid & (grid - 1) == 0 else (r - i) % grid

    def to_peer(block, r):
        return block if r == 0 else packed_send(block, "grid", lambda i: peer(i, r))

    sines = sine_table(length)
    peers = jnp.stack([jnp.asarray(peer(me, r), jnp.int32) for r in range(grid)])
    by_column = (peers[:, None] * columns + jnp.arange(columns)[None, :]).reshape(-1)
    by_plane = (
        peers[None, :, None] * planes
        + (jnp.arange(chunks) * width)[:, None, None]
        + jnp.arange(width)[None, None, :]
    ).reshape(-1)
    sines_y = sines[by_column]
    sines_x = sines[by_plane]

    mine = me if grid & (grid - 1) == 0 else peer(me, 0)
    modes = jnp.arange(1, length + 1, dtype=jnp.float32)
    local_modes = (mine * columns + jnp.arange(1, columns + 1, dtype=jnp.int32)).astype(jnp.float32)
    along_full = eigen_line(modes, length)
    along_local = eigen_line(local_modes, length)
    kernel = (2.0 / (length + 1)) ** 3 / (
        along_full[:, None, None]
        + along_local[None, :, None]
        + along_full[None, None, :]
        + screening
    )

    def pick(block, s):
        rows = []
        for i in range(per_group):
            row = block[0]
            for j in range(1, per_group):
                row = jnp.where(plan[s, i] == j, block[j], row)
            rows.append(row)
        return jnp.stack(rows)

    own, picked = [], []
    arrived = []
    for c in range(chunks):
        block = orbitals[:, c * width : (c + 1) * width]
        far = packed_send(block, "band", lambda i: (i - 2) % bands)
        near = packed_send(jnp.where(even, far, block), "band", lambda i: i ^ 1)
        chosen = jnp.concatenate([pick(near, 0), pick(far, 1)])
        both = jnp.concatenate([block, block])
        density = (both.astype(jnp.float32) * chosen.astype(jnp.float32)).astype(jnp.bfloat16)
        section = jnp.dot(density, sines, preferred_element_type=jnp.float32).astype(jnp.bfloat16)
        section = jnp.einsum(
            "pxyz,ky->pxkz", section, sines_y, preferred_element_type=jnp.float32
        ).astype(jnp.bfloat16)
        own.append(block)
        picked.append(chosen)
        for r in range(grid):
            arrived.append(to_peer(section[:, :, r * columns : (r + 1) * columns], r))

    pencils = jnp.concatenate(arrived, axis=1)
    spectrum = jnp.einsum("pxyz,xk->pkyz", pencils, sines_x, preferred_element_type=jnp.float32)
    scaled = (spectrum * kernel).astype(jnp.bfloat16)
    inverse = jnp.einsum(
        "pkyz,xk->pxyz", scaled, sines_x, preferred_element_type=jnp.float32
    ).astype(jnp.bfloat16)

    results = []
    for c in range(chunks):
        slabs = []
        for r in range(grid):
            start = (c * grid + r) * width
            slabs.append(to_peer(inverse[:, start : start + width], r))
        slab = jnp.concatenate(slabs, axis=2)
        slab = jnp.einsum(
            "pxyz,yk->pxkz", slab, sines_y, preferred_element_type=jnp.float32
        ).astype(jnp.bfloat16)
        potential = jnp.dot(slab, sines, preferred_element_type=jnp.float32)
        block = own[c].astype(jnp.float32)
        terms = potential * picked[c].astype(jnp.float32)
        total = terms[:per_group] + terms[per_group:]

        def partner_sum(s):
            weighted = potential[s * per_group : (s + 1) * per_group] * block
            return jnp.stack(
                [
                    sum(jnp.where(plan[s, i] == j, weighted[i], 0.0) for i in range(per_group))
                    for j in range(per_group)
                ]
            )

        swapped = packed_send(partner_sum(0).astype(jnp.bfloat16), "band", lambda i: i ^ 1)
        swapped = swapped.astype(jnp.float32)
        outgoing = partner_sum(1) + jnp.where(even, swapped, 0.0)
        returned = packed_send(outgoing.astype(jnp.bfloat16), "band", lambda i: (i + 2) % bands)
        total = total + jnp.where(even, 0.0, swapped) + returned.astype(jnp.float32)
        results.append((-total).astype(jnp.bfloat16))
    return jnp.concatenate(results, axis=1)


def dotf(a, b):
    return jnp.dot(a, b, preferred_element_type=jnp.float32)


def smem():
    return pl.BlockSpec(memory_space=pltpu.SMEM)


def whole(shape):
    return pl.BlockSpec(shape, lambda *_: (0,) * len(shape))


def params(n):
    return pltpu.CompilerParams(dimension_semantics=("arbitrary",) * n, vmem_limit_bytes=56 << 20)


STEP = 4


def pack_kernel(in_ref, order_ref, out_ref):
    length = in_ref.shape[-1]

    @pl.loop(0, out_ref.shape[1])
    def _(j):
        out_ref[0, j, :, :length] = in_ref[0, 2 * j]
        out_ref[0, j, :, length:] = in_ref[0, 2 * j + 1]


def pack(orbitals, spread, c):
    groups, _, _, length = orbitals.shape
    half = TILE // 2
    steps = half // STEP
    return pl.pallas_call(
        pack_kernel,
        grid=(groups, steps),
        in_specs=[
            pl.BlockSpec((1, 2 * STEP, length, length), lambda b, x: (b, c * steps + x, 0, 0)),
            whole(spread.shape),
        ],
        out_specs=pl.BlockSpec((1, STEP, length, 2 * length), lambda b, x: (b, x, 0, 0)),
        out_shape=jax.ShapeDtypeStruct((groups, half, length, 2 * length), jnp.bfloat16),
        compiler_params=params(2),
    )(orbitals, spread)


def mate_of(facts_ref, s, i, a_ref, b_ref):
    which = facts_ref[2 * s + i]
    return jnp.where(facts_ref[4] == 0, a_ref[which, 0].astype(jnp.float32), b_ref[which, 0].astype(jnp.float32))


def forward_kernel(s, grid, facts_ref, own_ref, a_ref, b_ref, sy_ref, lo_ref, hi_ref, swap_ref, *rest):
    outs, hold = rest[:grid], rest[grid]
    step = pl.program_id(0)
    half = TILE // 2
    wide = own_ref.shape[-1]
    rho = []
    for i in range(2):
        mate = mate_of(facts_ref, s, i, a_ref, b_ref)
        rho.append((own_ref[i, 0].astype(jnp.float32) * mate).astype(jnp.bfloat16))
    for part, table in ((0, lo_ref), (1, hi_ref)):
        lanes = slice(0, 256) if part == 0 else slice(wide - 256, wide)
        lhs = jnp.concatenate([rho[0][:, lanes], rho[1][:, lanes]], axis=1)
        along = dotf(lhs, table[...]).astype(jnp.bfloat16)
        hold[2 * step + part] = dotf(sy_ref[...], along).astype(jnp.bfloat16)

    @pl.when(step == half - 1)
    def _():
        per = outs[0].shape[0] // TILE
        for r in range(grid):
            for j in range(per):
                at = (r * per + j) * TILE
                block = hold[:, at : at + TILE, :].reshape(TILE * TILE, wide)
                block = dotf(swap_ref[...], block).astype(jnp.bfloat16)
                outs[r][j * TILE : (j + 1) * TILE] = block.reshape(TILE, TILE, wide)


def forward(s, facts, own, mates, tables, grid):
    half = TILE // 2
    _, _, length, wide = own.shape
    columns = length // grid
    field = pl.BlockSpec((2, 1, length, wide), lambda x: (0, x, 0, 0))
    piece = (columns, TILE, wide)
    held = [tables[k] for k in ("sy", "lo", "hi", "swap")]
    return pl.pallas_call(
        functools.partial(forward_kernel, s, grid),
        grid=(half,),
        in_specs=[smem(), field, field, field] + [whole(k.shape) for k in held],
        out_specs=[whole(piece)] * grid,
        out_shape=[jax.ShapeDtypeStruct(piece, jnp.bfloat16)] * grid,
        scratch_shapes=[pltpu.VMEM((TILE, length, wide), jnp.bfloat16)],
        compiler_params=params(1),
    )(facts, own, *mates, *held)


def middle_kernel(count, scale, per, line_ref, base_ref, sxt_ref, sx_ref, *rest):
    ins, outs = rest[:count], rest[count:]
    start = pl.program_id(0) * per
    for k in range(per):
        column = jnp.concatenate([ref[k] for ref in ins], axis=0)
        spectrum = dotf(sxt_ref[...], column)
        weight = scale / (base_ref[...] + line_ref[start + k])
        scaled = (spectrum * weight).astype(jnp.bfloat16)
        back = dotf(sx_ref[...], scaled).astype(jnp.bfloat16)
        for n, ref in enumerate(outs):
            ref[k] = back[n * TILE : (n + 1) * TILE]


def middle(pieces, tables):
    count = len(pieces)
    columns, _, wide = pieces[0].shape
    length = wide // 2
    per = 4
    piece = pl.BlockSpec((per, TILE, wide), lambda k: (k, 0, 0))
    return pl.pallas_call(
        functools.partial(middle_kernel, count, (2.0 / (length + 1)) ** 3, per),
        grid=(columns // per,),
        in_specs=[smem()] + [whole(tables[k].shape) for k in ("base", "sxt", "sx")] + [piece] * count,
        out_specs=[piece] * count,
        out_shape=[jax.ShapeDtypeStruct(pieces[0].shape, jnp.bfloat16)] * count,
        compiler_params=params(1),
    )(tables["line"], tables["base"], tables["sxt"], tables["sx"], *pieces)


def inverse_kernel(s, grid, facts_ref, own_ref, a_ref, b_ref, *rest):
    if s == 1:
        before_ref, back_ref, *rest = rest
    syt_ref, lo_ref, hi_ref, swap_ref = rest[:4]
    ins = rest[4 : 4 + grid]
    total_ref, sum_ref, hold = rest[4 + grid :]
    step = pl.program_id(0)
    wide = own_ref.shape[-1]

    @pl.when(step == 0)
    def _():
        per = ins[0].shape[0] // TILE
        for r in range(grid):
            for j in range(per):
                at = (r * per + j) * TILE
                block = ins[r][j * TILE : (j + 1) * TILE].reshape(TILE * TILE, wide)
                block = dotf(swap_ref[...], block).astype(jnp.bfloat16)
                hold[:, at : at + TILE, :] = block.reshape(TILE, TILE, wide)

    first = dotf(syt_ref[...], hold[2 * step]).astype(jnp.bfloat16)
    second = dotf(syt_ref[...], hold[2 * step + 1]).astype(jnp.bfloat16)
    weighted = []
    for i, table in ((0, lo_ref), (1, hi_ref)):
        lanes = slice(0, 256) if i == 0 else slice(wide - 256, wide)
        potential = dotf(jnp.concatenate([first[:, lanes], second[:, lanes]], axis=1), table[...])
        term = potential * mate_of(facts_ref, s, i, a_ref, b_ref)
        if s == 1:
            term = term + before_ref[i, 0] + back_ref[i, 0].astype(jnp.float32)
        total_ref[i, 0] = term
        weighted.append(potential * own_ref[i, 0].astype(jnp.float32))
    for j in range(2):
        parts = [jnp.where(facts_ref[2 * s + i] == j, weighted[i], 0.0) for i in range(2)]
        sum_ref[j, 0] = (parts[0] + parts[1]).astype(jnp.bfloat16)


def inverse(s, facts, own, mates, tables, pieces):
    grid = len(pieces)
    half = TILE // 2
    _, _, length, wide = own.shape
    field = pl.BlockSpec((2, 1, length, wide), lambda x: (0, x, 0, 0))
    held = [tables[k] for k in ("syt", "lo", "hi", "swap")]
    return pl.pallas_call(
        functools.partial(inverse_kernel, s, grid),
        grid=(half,),
        in_specs=[smem(), field]
        + [field] * len(mates)
        + [whole(k.shape) for k in held]
        + [whole(pieces[0].shape)] * grid,
        out_specs=[field, field],
        out_shape=[jax.ShapeDtypeStruct(own.shape, jnp.float32), jax.ShapeDtypeStruct(own.shape, jnp.bfloat16)],
        scratch_shapes=[pltpu.VMEM((TILE, length, wide), jnp.bfloat16)],
        compiler_params=params(1),
    )(facts, own, *mates, *held, *pieces)


def combine_kernel(a_ref, b_ref, out_ref):
    @pl.loop(0, out_ref.shape[1])
    def _(j):
        out_ref[0, j] = (a_ref[0, j].astype(jnp.float32) + b_ref[0, j].astype(jnp.float32)).astype(jnp.bfloat16)


def combine(a, b):
    spec = pl.BlockSpec((1, STEP) + a.shape[2:], lambda i, x: (i, x, 0, 0))
    return pl.pallas_call(
        combine_kernel,
        grid=(a.shape[0], a.shape[1] // STEP),
        in_specs=[spec, spec],
        out_specs=spec,
        out_shape=jax.ShapeDtypeStruct(a.shape, jnp.bfloat16),
        compiler_params=params(2),
    )(a, b)


def final_kernel(total_ref, near_ref, far_ref, gather_ref, *rest):
    out_ref = rest[-1]
    length = out_ref.shape[-1]

    @pl.loop(0, total_ref.shape[1])
    def _(j):
        total = total_ref[0, j] + near_ref[0, j].astype(jnp.float32) + far_ref[0, j].astype(jnp.float32)
        image = (-total).astype(jnp.bfloat16)
        out_ref[0, 2 * j] = image[:, :length]
        out_ref[0, 2 * j + 1] = image[:, length:]


def final(c, total, near, far, gather, shape, held):
    groups, half, length, wide = total.shape
    steps = half // STEP
    field = pl.BlockSpec((1, STEP, length, wide), lambda b, x: (b, x, 0, 0))
    extra = [] if held is None else [held]
    return pl.pallas_call(
        final_kernel,
        grid=(groups, steps),
        in_specs=[field, field, field, whole(gather.shape)] + [pl.BlockSpec(memory_space=pl.ANY)] * len(extra),
        out_specs=pl.BlockSpec((1, 2 * STEP, length, length), lambda b, x: (b, c * steps + x, 0, 0)),
        out_shape=jax.ShapeDtypeStruct(shape, jnp.bfloat16),
        input_output_aliases={4: 0} if extra else {},
        compiler_params=params(2),
    )(total, near, far, gather, *extra)


def gate_kernel(facts_ref, out_ref):
    for k in range(out_ref.shape[0]):
        out_ref[k] = facts_ref[k]


def gate(facts):
    return pl.pallas_call(
        gate_kernel, in_specs=[smem()], out_specs=smem(), out_shape=jax.ShapeDtypeStruct(facts.shape, jnp.int32)
    )(facts)


def after(value, *others):
    return lax.optimization_barrier((value,) + others)[0]


def shards(orbitals, plan):
    per_group, planes, _, length = orbitals.shape
    grid = lax.axis_size("grid")
    bands = lax.axis_size("band")
    columns = length // grid
    fits = planes % TILE == 0 and columns % TILE == 0 and length % 64 == 0 and 128 < length <= 192
    if per_group != 2 or bands % 2 or grid & (grid - 1) or plan.shape[0] != 2 or not fits:
        return plain_shards(orbitals, plan)
    me = lax.axis_index("grid")
    chunks = planes // TILE
    sines = sine_table(length)
    peers = jnp.stack([jnp.asarray(me ^ r, jnp.int32) for r in range(grid)])
    by_column = (peers[:, None] * columns + jnp.arange(columns)[None, :]).reshape(-1)
    by_plane = (
        peers[None, :, None] * planes + (jnp.arange(chunks) * TILE)[:, None, None] + jnp.arange(TILE)[None, None, :]
    ).reshape(-1)
    sy, sx = sines[by_column], sines[by_plane]
    full = eigen_line(jnp.arange(1, length + 1, dtype=jnp.float32), length)
    line = eigen_line((me * columns + jnp.arange(1, columns + 1, dtype=jnp.int32)).astype(jnp.float32), length)
    eye = jnp.eye(length, dtype=jnp.bfloat16)
    none = jnp.zeros_like(eye)
    gap = 256 - length

    def low(t):
        return jnp.pad(t, ((0, gap), (0, 0)))

    def high(t):
        return jnp.pad(t, ((gap, 0), (0, 0)))

    def split(place):
        top = jnp.concatenate([place(sines), place(none)], axis=1)
        bottom = jnp.concatenate([place(none), place(sines)], axis=1)
        return jnp.concatenate([top, bottom], axis=0)

    row = jnp.arange(TILE * TILE)
    swap = (row[:, None] == ((row % TILE) * TILE + row // TILE)[None, :]).astype(jnp.bfloat16)
    tables = {
        "sy": sy,
        "syt": sy.T,
        "sx": sx,
        "sxt": sx.T,
        "lo": split(low),
        "hi": split(high),
        "swap": swap,
        "line": line,
        "base": full[:, None] + jnp.concatenate([full, full])[None, :] + screening,
    }
    spread = jnp.concatenate([jnp.concatenate([eye, none], axis=1), jnp.concatenate([none, eye], axis=1)], axis=0)
    gather = high(eye)
    parity = (lax.axis_index("band") % 2).astype(jnp.int32)
    facts = jnp.concatenate([plan[1 - parity], plan[parity], parity[None]])

    def along(block, pairs):
        return lax.ppermute(block, "band", pairs)

    def exchange(pieces):
        got = [pieces[0]]
        for r in range(1, grid):
            got.append(lax.ppermute(pieces[r], "grid", [(i, i ^ r) for i in range(grid)]))
        return got

    down = [(i, (i - 2) % bands) for i in range(bands)]
    up = [(i, (i + 2) % bands) for i in range(bands)]

    own, far_even, near_even = [], [], []
    for c in range(chunks):
        if c == 1:
            tables = dict(zip(tables, lax.optimization_barrier(tuple(tables.values()))))
            spread = after(spread, own[0], *tables.values())
        elif c:
            spread = after(spread, own[-1])
        own.append(pack(orbitals, spread, c))
        far_even.append(along(own[c], down[0::2]))

    last = own[-1]
    sent, mates, turned = ([None] * chunks, [None] * chunks), ([], []), [None, None]
    totals, joined, done = [None] * chunks, [None] * chunks, [None] * chunks

    def front(s, c):
        nonlocal last
        pieces = forward(s, facts, after(own[c], last), mates[s][c], tables, grid)
        last = pieces[0]
        sent[s][c] = exchange(pieces)

    def turn(s):
        nonlocal last
        flat = [piece for c in range(chunks) for piece in sent[s][c]]
        flat[0] = after(flat[0], last)
        out = middle(flat, tables)
        last = out[0]
        turned[s] = [out[c * grid : (c + 1) * grid] for c in range(chunks)]

    def ending(s, c, behind=None):
        nonlocal last
        pieces = turned[s][c]
        if behind is not None:
            pieces = [after(piece, behind) for piece in pieces]
        got = exchange(pieces)
        got[0] = after(got[0], last)
        others = mates[s][c] if s == 0 else mates[s][c] + (totals[c], joined[c])
        totals[c], partner = inverse(s, facts, own[c], others, tables, got)
        last = partner
        if s == 0:
            joined[c] = (partner, along(partner, [(i, i ^ 1) for i in range(1, bands, 2)]))
        else:
            near = along(partner, [(i, i ^ 1) for i in range(0, bands, 2)])
            done[c] = (near, along(partner, up[1::2]))

    def join(c):
        nonlocal last
        partner, traded = joined[c]
        last = combine(after(partner, last), traded)
        joined[c] = along(last, up[0::2])

    for c in range(chunks):
        if c:
            facts = gate(after(facts, last))
        source = after(far_even[c], last if c == 0 else facts)
        near_odd = along(source, [(i, i ^ 1) for i in range(0, bands, 2)])
        mates[0].append((far_even[c], near_odd))
        front(0, c)
    for c in range(chunks):
        quiet = after(own[c], mates[0][-1][1])
        near_even = along(quiet, [(i, i ^ 1) for i in range(1, bands, 2)])
        mates[1].append((near_even, along(quiet, down[1::2])))
    front(1, 0)
    turn(0)
    for c in range(1, chunks):
        front(1, c)
        if c < chunks - 1:
            ending(0, c - 1)
    late = last
    for c in range(max(chunks - 2, 0), chunks):
        if c > 0:
            join(c - 1)
        if c == chunks - 1:
            turn(1)
        ending(0, c, late if c == chunks - 1 else None)
    join(chunks - 1)
    for c in range(chunks):
        ending(1, c)
    image = None
    for c, (near, far) in enumerate(done):
        image = final(c, after(totals[c], last), near, far, gather, orbitals.shape, image)
    return image


def solution(mesh):
    return jax.shard_map(
        shards,
        mesh=mesh,
        in_specs=(P("band", "grid", None, None), P(None, "band")),
        out_specs=P("band", "grid", None, None),
        check_vma=False,
    )
```

```python
import functools

import jax
import jax.numpy as jnp
from jax import lax
from jax.experimental import pallas as pl
from jax.experimental.pallas import tpu as pltpu
from jax.sharding import PartitionSpec as P


CHUNKS = 4
PACK = True

screening = 0.0005
TILE = 16


def routed(block, axis, target):
    return lax.ppermute(block, axis, [(i, target(i)) for i in range(lax.axis_size(axis))])


def packed_send(block, axis, target):
    parts = block.shape[0]
    length = block.shape[-1]
    if not PACK or length % 128 == 0 or (2 * length) % 128 or parts % 2:
        return routed(block, axis, target)
    half = parts // 2
    wide = jnp.concatenate([block[:half], block[half:]], axis=-1)
    got = routed(wide, axis, target)
    return jnp.concatenate([got[..., :length], got[..., length:]], axis=0)


def sine_table(length):
    counts = jnp.arange(1, length + 1, dtype=jnp.float32)
    return jnp.sin(jnp.pi * counts[:, None] * counts[None, :] / (length + 1)).astype(jnp.bfloat16)


def eigen_line(modes, length):
    return 2.0 - 2.0 * jnp.cos(jnp.pi * modes / (length + 1))


def plain_shards(orbitals, plan):
    per_group, planes, _, length = orbitals.shape
    grid = lax.axis_size("grid")
    bands = lax.axis_size("band")
    me = lax.axis_index("grid")
    even = lax.axis_index("band") % 2 == 0
    columns = length // grid
    chunks = CHUNKS if planes % CHUNKS == 0 else 1
    width = planes // chunks

    def peer(i, r):
        return i ^ r if grid & (grid - 1) == 0 else (r - i) % grid

    def to_peer(block, r):
        return block if r == 0 else packed_send(block, "grid", lambda i: peer(i, r))

    sines = sine_table(length)
    peers = jnp.stack([jnp.asarray(peer(me, r), jnp.int32) for r in range(grid)])
    by_column = (peers[:, None] * columns + jnp.arange(columns)[None, :]).reshape(-1)
    by_plane = (
        peers[None, :, None] * planes
        + (jnp.arange(chunks) * width)[:, None, None]
        + jnp.arange(width)[None, None, :]
    ).reshape(-1)
    sines_y = sines[by_column]
    sines_x = sines[by_plane]

    mine = me if grid & (grid - 1) == 0 else peer(me, 0)
    modes = jnp.arange(1, length + 1, dtype=jnp.float32)
    local_modes = (mine * columns + jnp.arange(1, columns + 1, dtype=jnp.int32)).astype(jnp.float32)
    along_full = eigen_line(modes, length)
    along_local = eigen_line(local_modes, length)
    kernel = (2.0 / (length + 1)) ** 3 / (
        along_full[:, None, None]
        + along_local[None, :, None]
        + along_full[None, None, :]
        + screening
    )

    def pick(block, s):
        rows = []
        for i in range(per_group):
            row = block[0]
            for j in range(1, per_group):
                row = jnp.where(plan[s, i] == j, block[j], row)
            rows.append(row)
        return jnp.stack(rows)

    own, picked = [], []
    arrived = []
    for c in range(chunks):
        block = orbitals[:, c * width : (c + 1) * width]
        far = packed_send(block, "band", lambda i: (i - 2) % bands)
        near = packed_send(jnp.where(even, far, block), "band", lambda i: i ^ 1)
        chosen = jnp.concatenate([pick(near, 0), pick(far, 1)])
        both = jnp.concatenate([block, block])
        density = (both.astype(jnp.float32) * chosen.astype(jnp.float32)).astype(jnp.bfloat16)
        section = jnp.dot(density, sines, preferred_element_type=jnp.float32).astype(jnp.bfloat16)
        section = jnp.einsum(
            "pxyz,ky->pxkz", section, sines_y, preferred_element_type=jnp.float32
        ).astype(jnp.bfloat16)
        own.append(block)
        picked.append(chosen)
        for r in range(grid):
            arrived.append(to_peer(section[:, :, r * columns : (r + 1) * columns], r))

    pencils = jnp.concatenate(arrived, axis=1)
    spectrum = jnp.einsum("pxyz,xk->pkyz", pencils, sines_x, preferred_element_type=jnp.float32)
    scaled = (spectrum * kernel).astype(jnp.bfloat16)
    inverse = jnp.einsum(
        "pkyz,xk->pxyz", scaled, sines_x, preferred_element_type=jnp.float32
    ).astype(jnp.bfloat16)

    results = []
    for c in range(chunks):
        slabs = []
        for r in range(grid):
            start = (c * grid + r) * width
            slabs.append(to_peer(inverse[:, start : start + width], r))
        slab = jnp.concatenate(slabs, axis=2)
        slab = jnp.einsum(
            "pxyz,yk->pxkz", slab, sines_y, preferred_element_type=jnp.float32
        ).astype(jnp.bfloat16)
        potential = jnp.dot(slab, sines, preferred_element_type=jnp.float32)
        block = own[c].astype(jnp.float32)
        terms = potential * picked[c].astype(jnp.float32)
        total = terms[:per_group] + terms[per_group:]

        def partner_sum(s):
            weighted = potential[s * per_group : (s + 1) * per_group] * block
            return jnp.stack(
                [
                    sum(jnp.where(plan[s, i] == j, weighted[i], 0.0) for i in range(per_group))
                    for j in range(per_group)
                ]
            )

        swapped = packed_send(partner_sum(0).astype(jnp.bfloat16), "band", lambda i: i ^ 1)
        swapped = swapped.astype(jnp.float32)
        outgoing = partner_sum(1) + jnp.where(even, swapped, 0.0)
        returned = packed_send(outgoing.astype(jnp.bfloat16), "band", lambda i: (i + 2) % bands)
        total = total + jnp.where(even, 0.0, swapped) + returned.astype(jnp.float32)
        results.append((-total).astype(jnp.bfloat16))
    return jnp.concatenate(results, axis=1)


def dotf(a, b):
    return jnp.dot(a, b, preferred_element_type=jnp.float32)


def smem():
    return pl.BlockSpec(memory_space=pltpu.SMEM)


def whole(shape):
    return pl.BlockSpec(shape, lambda *_: (0,) * len(shape))


def params(n):
    return pltpu.CompilerParams(dimension_semantics=("arbitrary",) * n, vmem_limit_bytes=56 << 20)


STEP = 4


def pack_kernel(in_ref, order_ref, out_ref):
    length = in_ref.shape[-1]

    @pl.loop(0, out_ref.shape[1])
    def _(j):
        out_ref[0, j, :, :length] = in_ref[0, 2 * j]
        out_ref[0, j, :, length:] = in_ref[0, 2 * j + 1]


def pack(orbitals, spread, c):
    groups, _, _, length = orbitals.shape
    half = TILE // 2
    steps = half // STEP
    return pl.pallas_call(
        pack_kernel,
        grid=(groups, steps),
        in_specs=[
            pl.BlockSpec((1, 2 * STEP, length, length), lambda b, x: (b, c * steps + x, 0, 0)),
            whole(spread.shape),
        ],
        out_specs=pl.BlockSpec((1, STEP, length, 2 * length), lambda b, x: (b, x, 0, 0)),
        out_shape=jax.ShapeDtypeStruct((groups, half, length, 2 * length), jnp.bfloat16),
        compiler_params=params(2),
    )(orbitals, spread)


def mate_of(facts_ref, s, i, a_ref, b_ref):
    which = facts_ref[2 * s + i]
    return a_ref[which, 0] + b_ref[which, 0]


def fields(length, wide):
    shape = (2, 1, length, wide)
    return (
        pl.BlockSpec(shape, lambda x, facts: (0, x, 0, 0)),
        pl.BlockSpec(shape, lambda x, facts: (0, x * (1 - facts[4]), 0, 0)),
        pl.BlockSpec(shape, lambda x, facts: (0, x * facts[4], 0, 0)),
    )


def gridded(steps, in_specs, out_specs, scratch):
    return pltpu.PrefetchScalarGridSpec(
        num_scalar_prefetch=1, grid=(steps,), in_specs=in_specs, out_specs=out_specs, scratch_shapes=scratch
    )


def forward_kernel(s, grid, facts_ref, own_ref, a_ref, b_ref, sy_ref, lo_ref, hi_ref, swap_ref, *rest):
    outs, hold = rest[:grid], rest[grid]
    step = pl.program_id(0)
    half = TILE // 2
    wide = own_ref.shape[-1]
    rho = []
    for i in range(2):
        rho.append(own_ref[i, 0] * mate_of(facts_ref, s, i, a_ref, b_ref))
    for part, table in ((0, lo_ref), (1, hi_ref)):
        lanes = slice(0, 256) if part == 0 else slice(wide - 256, wide)
        lhs = jnp.concatenate([rho[0][:, lanes], rho[1][:, lanes]], axis=1)
        along = dotf(lhs, table[...]).astype(jnp.bfloat16)
        hold[2 * step + part] = dotf(sy_ref[...], along).astype(jnp.bfloat16)

    @pl.when(step == half - 1)
    def _():
        per = outs[0].shape[0] // TILE
        for r in range(grid):
            for j in range(per):
                at = (r * per + j) * TILE
                block = hold[:, at : at + TILE, :].reshape(TILE * TILE, wide)
                block = dotf(swap_ref[...], block).astype(jnp.bfloat16)
                outs[r][j * TILE : (j + 1) * TILE] = block.reshape(TILE, TILE, wide)


def forward(s, facts, own, mates, tables, grid):
    half = TILE // 2
    _, _, length, wide = own.shape
    columns = length // grid
    piece = (columns, TILE, wide)
    held = [tables[k] for k in ("sy", "lo", "hi", "swap")]
    return pl.pallas_call(
        functools.partial(forward_kernel, s, grid),
        grid_spec=gridded(
            half,
            list(fields(length, wide)) + [whole(k.shape) for k in held],
            [whole(piece)] * grid,
            [pltpu.VMEM((TILE, length, wide), jnp.bfloat16)],
        ),
        out_shape=[jax.ShapeDtypeStruct(piece, jnp.bfloat16)] * grid,
        compiler_params=params(1),
    )(facts, own, *mates, *held)


def middle_kernel(count, per, line_ref, base_ref, sxt_ref, sx_ref, *rest):
    ins, outs = rest[:count], rest[count:]
    start = pl.program_id(0) * per

    @pl.loop(0, per, step=2)
    def _(at):
        for k in (at, at + 1):
            column = jnp.concatenate([ref[k] for ref in ins], axis=0)
            spectrum = dotf(sxt_ref[...], column)
            weight = pl.reciprocal(base_ref[...] + line_ref[start + k], approx=False)
            back = dotf(sx_ref[...], (spectrum * weight).astype(jnp.bfloat16)).astype(jnp.bfloat16)
            for n, ref in enumerate(outs):
                ref[k] = back[n * TILE : (n + 1) * TILE]


def middle(pieces, tables):
    count = len(pieces)
    columns, _, wide = pieces[0].shape
    per = 8
    piece = pl.BlockSpec((per, TILE, wide), lambda k: (k, 0, 0))
    return pl.pallas_call(
        functools.partial(middle_kernel, count, per),
        grid=(columns // per,),
        in_specs=[smem()] + [whole(tables[k].shape) for k in ("base", "sxt", "sx")] + [piece] * count,
        out_specs=[piece] * count,
        out_shape=[jax.ShapeDtypeStruct(pieces[0].shape, jnp.bfloat16)] * count,
        compiler_params=params(1),
    )(tables["line"], tables["base"], tables["sxt"], tables["sx"], *pieces)


def inverse_kernel(s, grid, facts_ref, own_ref, a_ref, b_ref, *rest):
    if s == 1:
        before_ref, back_ref, *rest = rest
    syt_ref, lo_ref, hi_ref, swap_ref = rest[:4]
    ins = rest[4 : 4 + grid]
    total_ref, sum_ref, hold = rest[4 + grid :]
    step = pl.program_id(0)
    wide = own_ref.shape[-1]

    @pl.when(step == 0)
    def _():
        per = ins[0].shape[0] // TILE
        for r in range(grid):
            for j in range(per):
                at = (r * per + j) * TILE
                block = ins[r][j * TILE : (j + 1) * TILE].reshape(TILE * TILE, wide)
                block = dotf(swap_ref[...], block).astype(jnp.bfloat16)
                hold[:, at : at + TILE, :] = block.reshape(TILE, TILE, wide)

    first = dotf(syt_ref[...], hold[2 * step]).astype(jnp.bfloat16)
    second = dotf(syt_ref[...], hold[2 * step + 1]).astype(jnp.bfloat16)
    weighted = []
    for i, table in ((0, lo_ref), (1, hi_ref)):
        lanes = slice(0, 256) if i == 0 else slice(wide - 256, wide)
        potential = dotf(jnp.concatenate([first[:, lanes], second[:, lanes]], axis=1), table[...])
        term = potential * mate_of(facts_ref, s, i, a_ref, b_ref).astype(jnp.float32)
        if s == 1:
            term = term + before_ref[i, 0].astype(jnp.float32) + back_ref[i, 0].astype(jnp.float32)
        total_ref[i, 0] = term.astype(jnp.bfloat16)
        weighted.append(potential * own_ref[i, 0].astype(jnp.float32))
    which = facts_ref[2 * s]
    shared = (facts_ref[2 * s + 1] == which).astype(jnp.float32)
    sum_ref[which, 0] = (weighted[0] + shared * weighted[1]).astype(jnp.bfloat16)
    sum_ref[1 - which, 0] = ((1.0 - shared) * weighted[1]).astype(jnp.bfloat16)


def inverse(s, facts, own, mates, tables, pieces):
    grid = len(pieces)
    half = TILE // 2
    _, _, length, wide = own.shape
    held = [tables[k] for k in ("syt", "lo", "hi", "swap")]
    field, a_field, b_field = fields(length, wide)
    return pl.pallas_call(
        functools.partial(inverse_kernel, s, grid),
        grid_spec=gridded(
            half,
            [field, a_field, b_field]
            + [field] * (len(mates) - 2)
            + [whole(k.shape) for k in held]
            + [whole(pieces[0].shape)] * grid,
            [field, field],
            [pltpu.VMEM((TILE, length, wide), jnp.bfloat16)],
        ),
        out_shape=[jax.ShapeDtypeStruct(own.shape, jnp.bfloat16)] * 2,
        compiler_params=params(1),
    )(facts, own, *mates, *held, *pieces)


def final_kernel(total_ref, near_ref, far_ref, *rest):
    out_ref = rest[-1]
    length = out_ref.shape[-1]

    @pl.loop(0, total_ref.shape[1])
    def _(j):
        total = total_ref[0, j].astype(jnp.float32) + near_ref[0, j].astype(jnp.float32) + far_ref[0, j].astype(jnp.float32)
        image = (-total).astype(jnp.bfloat16)
        out_ref[0, 2 * j] = image[:, :length]
        out_ref[0, 2 * j + 1] = image[:, length:]


def final(c, total, near, far, shape, held):
    groups, half, length, wide = total.shape
    steps = half // STEP
    field = pl.BlockSpec((1, STEP, length, wide), lambda b, x: (b, x, 0, 0))
    extra = [] if held is None else [held]
    return pl.pallas_call(
        final_kernel,
        grid=(groups, steps),
        in_specs=[field, field, field] + [pl.BlockSpec(memory_space=pl.ANY)] * len(extra),
        out_specs=pl.BlockSpec((1, 2 * STEP, length, length), lambda b, x: (b, c * steps + x, 0, 0)),
        out_shape=jax.ShapeDtypeStruct(shape, jnp.bfloat16),
        input_output_aliases={3: 0} if extra else {},
        compiler_params=params(2),
    )(total, near, far, *extra)


def gate_kernel(facts_ref, out_ref):
    for k in range(out_ref.shape[0]):
        out_ref[k] = facts_ref[k]


def gate(facts):
    return pl.pallas_call(
        gate_kernel,
        in_specs=[smem()],
        out_specs=smem(),
        out_shape=jax.ShapeDtypeStruct(facts.shape, jnp.int32),
    )(facts)


def after(value, *others):
    return lax.optimization_barrier((value,) + others)[0]


def shards(orbitals, plan):
    per_group, planes, _, length = orbitals.shape
    grid = lax.axis_size("grid")
    bands = lax.axis_size("band")
    columns = length // grid
    fits = planes % TILE == 0 and columns % TILE == 0 and length % 64 == 0 and 128 < length <= 192
    if per_group != 2 or bands % 2 or grid & (grid - 1) or plan.shape[0] != 2 or not fits:
        return plain_shards(orbitals, plan)
    me = lax.axis_index("grid")
    chunks = planes // TILE
    sines = sine_table(length)
    peers = jnp.stack([jnp.asarray(me ^ r, jnp.int32) for r in range(grid)])
    by_column = (peers[:, None] * columns + jnp.arange(columns)[None, :]).reshape(-1)
    by_plane = (
        peers[None, :, None] * planes + (jnp.arange(chunks) * TILE)[:, None, None] + jnp.arange(TILE)[None, None, :]
    ).reshape(-1)
    sy, sx = sines[by_column], sines[by_plane]
    full = eigen_line(jnp.arange(1, length + 1, dtype=jnp.float32), length)
    line = eigen_line((me * columns + jnp.arange(1, columns + 1, dtype=jnp.int32)).astype(jnp.float32), length)
    scale = (2.0 / (length + 1)) ** 3
    eye = jnp.eye(length, dtype=jnp.bfloat16)
    none = jnp.zeros_like(eye)
    gap = 256 - length

    def low(t):
        return jnp.pad(t, ((0, gap), (0, 0)))

    def high(t):
        return jnp.pad(t, ((gap, 0), (0, 0)))

    def split(place):
        top = jnp.concatenate([place(sines), place(none)], axis=1)
        bottom = jnp.concatenate([place(none), place(sines)], axis=1)
        return jnp.concatenate([top, bottom], axis=0)

    row = jnp.arange(TILE * TILE)
    swap = (row[:, None] == ((row % TILE) * TILE + row // TILE)[None, :]).astype(jnp.bfloat16)
    tables = {
        "sy": sy,
        "syt": sy.T,
        "sx": sx,
        "sxt": sx.T,
        "lo": split(low),
        "hi": split(high),
        "swap": swap,
        "line": line / scale,
        "base": (full[:, None] + jnp.concatenate([full, full])[None, :] + screening) / scale,
    }
    spread = jnp.concatenate([jnp.concatenate([eye, none], axis=1), jnp.concatenate([none, eye], axis=1)], axis=0)
    parity = (lax.axis_index("band") % 2).astype(jnp.int32)
    facts = jnp.concatenate([plan[1 - parity], plan[parity], parity[None]])

    def along(block, pairs):
        return lax.ppermute(block, "band", pairs)

    def exchange(pieces):
        got = [pieces[0]]
        for r in range(1, grid):
            got.append(lax.ppermute(pieces[r], "grid", [(i, i ^ r) for i in range(grid)]))
        return got

    down = [(i, (i - 2) % bands) for i in range(bands)]
    up = [(i, (i + 2) % bands) for i in range(bands)]

    own, far_even, near_even = [], [], []
    for c in range(chunks):
        if c == 1:
            tables = dict(zip(tables, lax.optimization_barrier(tuple(tables.values()))))
            spread = after(spread, own[0], *tables.values())
        elif c:
            spread = after(spread, own[-1])
        own.append(pack(orbitals, spread, c))
        far_even.append(along(own[c], down[0::2]))

    last = own[-1]
    sent, mates, turned = ([None] * chunks, [None] * chunks), ([], []), [None, None]
    totals, joined, done = [None] * chunks, [None] * chunks, [None] * chunks

    def front(s, c):
        nonlocal last
        pieces = forward(s, facts, after(own[c], last), mates[s][c], tables, grid)
        last = pieces[0]
        sent[s][c] = exchange(pieces)

    def turn(s):
        nonlocal last
        flat = [piece for c in range(chunks) for piece in sent[s][c]]
        flat[0] = after(flat[0], last)
        out = middle(flat, tables)
        last = out[0]
        turned[s] = [out[c * grid : (c + 1) * grid] for c in range(chunks)]

    def ending(s, c, behind=None):
        nonlocal last
        pieces = turned[s][c]
        if behind is not None:
            pieces = [after(piece, behind) for piece in pieces]
        got = exchange(pieces)
        got[0] = after(got[0], last)
        others = mates[s][c] if s == 0 else mates[s][c] + (totals[c], joined[c])
        totals[c], partner = inverse(s, facts, own[c], others, tables, got)
        last = partner
        if s == 0:
            joined[c] = (partner, along(partner, [(i, i ^ 1) for i in range(1, bands, 2)]))
        else:
            near = along(partner, [(i, i ^ 1) for i in range(0, bands, 2)])
            done[c] = (near, along(partner, up[1::2]))

    def join(c):
        nonlocal last
        partner, traded = joined[c]
        first = after(partner, last).astype(jnp.float32)
        last = (first + traded.astype(jnp.float32)).astype(jnp.bfloat16)
        joined[c] = along(last, up[0::2])

    for c in range(chunks):
        if c:
            facts = gate(after(facts, last))
        source = after(far_even[c], last if c == 0 else facts)
        near_odd = along(source, [(i, i ^ 1) for i in range(0, bands, 2)])
        mates[0].append((far_even[c], near_odd))
        front(0, c)
    for c in range(chunks):
        quiet = after(own[c], mates[0][-2 if c == 0 and chunks > 1 else -1][1])
        near_even = along(quiet, [(i, i ^ 1) for i in range(1, bands, 2)])
        mates[1].append((near_even, along(quiet, down[1::2])))
    front(1, 0)
    turn(0)
    for c in range(1, chunks):
        front(1, c)
        if c < chunks - 1:
            ending(0, c - 1)
    late = last
    for c in range(max(chunks - 2, 0), chunks):
        if c > 0:
            join(c - 1)
        if c == chunks - 1:
            turn(1)
        ending(0, c, late if c == chunks - 1 else None)
    join(chunks - 1)
    for c in range(chunks):
        ending(1, c)
    image = None
    for c, (near, far) in enumerate(done):
        image = final(c, after(totals[c], last), near, far, orbitals.shape, image)
    return image


def solution(mesh):
    return jax.shard_map(
        shards,
        mesh=mesh,
        in_specs=(P("band", "grid", None, None), P(None, "band")),
        out_specs=P("band", "grid", None, None),
        check_vma=False,
    )
```
